32 devices in a mesh: group: 4 (over y, core), replica: 8 (over z, x).
Axes of the slice: x: 2, y: 2, z: 4, core: 2. Of those that a mesh axis runs over, the one named last changes fastest.
Arguments:
- inputs: bfloat16 [32, 128, 1600], P(('group', 'replica')), may hold values from -6 to 6
- segments: int32 [32, 128], P(('group', 'replica')), may hold values from 0 to 3, never falling along the last dimension, each value on 1 to 64 neighbouring positions
- cotangent: bfloat16 [32, 128, 1600], P(('group', 'replica')), may hold values from -6 to 6
- norm1_gain: bfloat16 [1600], P('group'), may hold values from 0.5 to 1.5
- norm1_bias: bfloat16 [1600], P('group'), may hold values from -3 to 3
- w_qkv: bfloat16 [1600, 4800], P('group'), may hold values from -8 to 8
- bias_qv: bfloat16 [3200], P('group'), may hold values from -3 to 3
- w_out: bfloat16 [1600, 1600], P('group'), may hold values from -0.625 to 0.625
- bias_out: bfloat16 [1600], P('group'), may hold values from -3 to 3
- norm2_gain: bfloat16 [1600], P('group'), may hold values from 0.5 to 1.5
- norm2_bias: bfloat16 [1600], P('group'), may hold values from -3 to 3
- w_fc: bfloat16 [1600, 6400], P('group'), may hold values from -0.15625 to 0.15625
- bias_fc: bfloat16 [6400], P('group'), may hold values from -3 to 3
- w_proj: bfloat16 [6400, 1600], P('group'), may hold values from -0.078125 to 0.078125
- bias_proj: bfloat16 [1600], P('group'), may hold values from -3 to 3
Outputs:
- outputs: bfloat16 [32, 128, 1600], P(('group', 'replica'))
- input_grad: float32 [32, 128, 1600], P(('group', 'replica'))
- grad_norm1_gain: float32 [1600], P('group')
- grad_norm1_bias: float32 [1600], P('group')
- grad_w_qkv: float32 [1600, 4800], P('group')
- grad_bias_qv: float32 [3200], P('group')
- grad_w_out: float32 [1600, 1600], P('group')
- grad_bias_out: float32 [1600], P('group')
- grad_norm2_gain: float32 [1600], P('group')
- grad_norm2_bias: float32 [1600], P('group')
- grad_w_fc: float32 [1600, 6400], P('group')
- grad_bias_fc: float32 [6400], P('group')
- grad_w_proj: float32 [6400, 1600], P('group')
- grad_bias_proj: float32 [1600], P('group')
The draws below stay inside these ranges and needn't reach their ends.
Inputs may be any that keep to these rules, and one draw needn't show every extreme that they name: `segments`: each packed row's segment numbers never fall; a segment holds 1 to 64 tokens, and some segment holds exactly that many.
All inputs are finite; a program needn't handle non-finite values.
Results may differ from the reference program's by a relative error of at most 0.0095.
Values may be sent and summed in bfloat16 or wider, within the bound.
A program may use at most 640 MiB of HBM per device.

```python
import math
import jax
import jax.numpy as jnp
import numpy as np
from jax import lax

D = 1600
HEAD_DIM = 64
FF = 6400
TOK_DEV = 128
ROWS = 32


def draw_w_qkv(key, part):
    spread = D ** (-0.5)
    base = jax.random.normal(key, (D, 3 * D), jnp.float32) * spread
    base = jnp.clip(base, -6.0 * spread, 6.0 * spread)
    return base.astype(jnp.bfloat16)


def level_of(stream_key, shape, pieces, smallest, high):
    factor_of, own = 1.0, jax.random.fold_in(stream_key, 6)
    for position, blocks in pieces:
        steps = jnp.exp(jax.random.uniform(jax.random.fold_in(own, position), (blocks,), jnp.float32, smallest / len(pieces), high / len(pieces)))
        factor_of = factor_of * jnp.repeat(steps, shape[position] // blocks).reshape([-1 if axis == position else 1 for axis in range(len(shape))])
    return factor_of


def split_up(count, total, reach, skew):
    portions = [(1 << 20) // math.isqrt(rank ** skew) + 1 for rank in range(2, count + 1)]
    surplus, given = total - reach - (count - 1), [1] * (count - 1)
    while surplus > 0:
        movable = [i for i in range(count - 1) if given[i] < reach]
        mass, left = sum([portions[i] for i in movable]), surplus
        for i in movable:
            addition = min(reach - given[i], max(1, left * portions[i] // mass), surplus)
            given[i] = given[i] + addition
            surplus = surplus - addition
    return np.array([reach] + given)


def ragged_sizes(rng, amount, total, most, lean):
    if amount == 2:
        one = jax.random.randint(rng, (), max(1, total - most), min(most, total - 1) + 1)
        return jnp.stack([one, total - one])
    lengths = jnp.asarray(split_up(amount, total, most, lean), jnp.int32)
    couples = (amount - 1) // 2
    donor, sink = lengths[1:1 + 2 * couples:2], lengths[2:2 + 2 * couples:2]
    room = jnp.minimum(donor - 1, most - sink)
    passed = jax.random.randint(jax.random.fold_in(rng, 1), (couples,), 0, 1 << 20) % (room + 1)
    lengths = lengths.at[1:1 + 2 * couples:2].set(donor - passed).at[2:2 + 2 * couples:2].set(sink + passed)
    return lengths[jax.random.permutation(jax.random.fold_in(rng, 2), amount)]


def normal_values(stream_key, dims, deviation, limit, cuts=(), dtype=jnp.bfloat16):
    array = deviation * jax.random.normal(stream_key, dims, jnp.float32)
    if cuts:
        array = array * level_of(stream_key, dims, cuts, -0.22, 0.18)
    return jnp.clip(array, -limit, limit).astype(dtype)


def setup_inputs(seed: int = 0) -> dict:
    splits = jax.random.split(jax.random.key(seed), 16)
    return {
        "inputs": normal_values(splits[0], (ROWS, TOK_DEV, D), 1.0, 6.0, ((0, 32),)),
        "segments": jax.vmap(lambda own: jnp.searchsorted(jnp.cumsum(ragged_sizes(own, 4, TOK_DEV, TOK_DEV // 2, 0)), jnp.arange(TOK_DEV), side="right"))(jax.random.split(splits[1], ROWS)).reshape((ROWS, TOK_DEV)).astype(jnp.int32),
        "cotangent": normal_values(splits[2], (ROWS, TOK_DEV, D), 1.0, 6.0, ((0, 32),)),
        "norm1_gain": jnp.clip(1.0 + 0.1 * jax.random.normal(splits[3], (D,), jnp.float32), 0.5, 1.5).astype(jnp.bfloat16),
        "norm1_bias": normal_values(splits[4], (D,), 0.3, 3.0, ((0, 4),)),
        "w_qkv": draw_w_qkv(jax.random.fold_in(splits[15], 71), 0),
        "bias_qv": normal_values(splits[6], (2 * D,), 0.3, 3.0, ((0, 4),)),
        "w_out": normal_values(splits[7], (D, D), (D // 16) ** -0.5, 0.625, ((0, 4),)),
        "bias_out": normal_values(splits[8], (D,), 0.3, 3.0, ((0, 4),)),
        "norm2_gain": jnp.clip(1.0 + 0.1 * jax.random.normal(splits[9], (D,), jnp.float32), 0.5, 1.5).astype(jnp.bfloat16),
        "norm2_bias": normal_values(splits[10], (D,), 0.3, 3.0, ((0, 4),)),
        "w_fc": normal_values(splits[11], (D, FF), D ** -0.5, 0.15625, ((0, 4),)),
        "bias_fc": normal_values(splits[12], (FF,), 0.3, 3.0, ((0, 4),)),
        "w_proj": normal_values(splits[13], (FF, D), FF ** -0.5, 0.078125, ((0, 4),)),
        "bias_proj": normal_values(splits[14], (D,), 0.3, 3.0, ((0, 4),)),
    }


EPSILON = 1e-05
GELU_SCALE = 0.7978845608028654
CUBIC_TERM = 0.044715

def matmul_plain(left_side, right_side):
    return jnp.dot(left_side, right_side, preferred_element_type=jnp.float32)

def matmul_left(left_side, right_side):
    return lax.dot_general(left_side.astype(jnp.float32), right_side.astype(jnp.float32), (((0,), (0,)), ((), ())))

def matmul_right(left_side, right_side):
    return lax.dot_general(left_side.astype(jnp.float32), right_side.astype(jnp.float32), (((1,), (1,)), ((), ())))

def batched(form, left_side, right_side):
    return jnp.einsum(form, left_side.astype(jnp.float32), right_side.astype(jnp.float32))

def norm_forward(values, norm_gain, offset):
    center = values - lax.optimization_barrier(jnp.mean(values, axis=-1, keepdims=True))
    inverse = lax.rsqrt(lax.optimization_barrier(jnp.mean(center * center, axis=-1, keepdims=True)) + EPSILON)
    scaled = center * inverse
    return (scaled * norm_gain + offset, scaled, inverse)

def norm_backward(upstream, scaled, inverse, norm_gain):
    weighted = upstream * norm_gain
    result = inverse * (weighted - lax.optimization_barrier(jnp.mean(weighted, axis=-1, keepdims=True)) - scaled * lax.optimization_barrier(jnp.mean(weighted * scaled, axis=-1, keepdims=True)))
    return (result, lax.optimization_barrier(jnp.sum(upstream * scaled, axis=0)), lax.optimization_barrier(jnp.sum(upstream, axis=0)))

def gelu_tanh(values):
    tangent = jnp.tanh(GELU_SCALE * (values + CUBIC_TERM * values * values * values))
    return 0.5 * values * (1.0 + tangent)

def gelu_slope(values):
    tangent = jnp.tanh(GELU_SCALE * (values + CUBIC_TERM * values * values * values))
    return 0.5 * (1.0 + tangent) + 0.5 * values * (1.0 - tangent * tangent) * GELU_SCALE * (1.0 + 3.0 * CUBIC_TERM * values * values)

def allowed_mask(segments):
    positions = jnp.arange(segments.shape[1])
    causal = positions[:, None] >= positions[None, :]
    same_segment = segments[:, :, None] == segments[:, None, :]
    return (same_segment & causal[None, :, :])[:, None, :, :]

def masked_scores(queries, keyed, allowed):
    raw = batched('rqhd,rkhd->rhqk', queries, keyed) * HEAD_DIM ** (-0.5)
    return jnp.where(allowed, raw, -1e+30)

def layer_forward(inputs, segments, params):
    norm1_gain, norm1_bias, w_qkv, bias_qv, w_out, bias_out, norm2_gain, norm2_bias, w_fc, bias_fc, w_proj, bias_proj = params
    row_count, length, feature_width = inputs.shape
    head_count = feature_width // HEAD_DIM
    tokens = inputs.reshape(row_count * length, feature_width).astype(jnp.float32)
    first_norm, first_scaled, first_inverse = norm_forward(tokens, norm1_gain.astype(jnp.float32), norm1_bias.astype(jnp.float32))
    first_cast = first_norm.astype(jnp.bfloat16)
    qkv_bias = jnp.concatenate([bias_qv[:feature_width].astype(jnp.float32), jnp.zeros((feature_width,), jnp.float32), bias_qv[feature_width:].astype(jnp.float32)])
    projected = (matmul_plain(first_cast, w_qkv) + qkv_bias).astype(jnp.bfloat16)
    split_qkv = projected.reshape(row_count, length, 3, head_count, HEAD_DIM)
    queries, keyed, values = (split_qkv[:, :, 0], split_qkv[:, :, 1], split_qkv[:, :, 2])
    allowed = allowed_mask(segments)
    scores = masked_scores(queries, keyed, allowed)
    row_peak = lax.optimization_barrier(jnp.max(scores, axis=-1, keepdims=True))
    logsum = row_peak + jnp.log(lax.optimization_barrier(jnp.sum(jnp.exp(scores - row_peak), axis=-1, keepdims=True)))
    attn_probs = jnp.exp(scores - logsum).astype(jnp.bfloat16)
    attended = batched('rhqk,rkhd->rqhd', attn_probs, values).reshape(row_count * length, feature_width)
    attended_cast = attended.astype(jnp.bfloat16)
    residual = tokens + matmul_plain(attended_cast, w_out) + bias_out.astype(jnp.float32)
    second_norm, second_scaled, second_inverse = norm_forward(residual, norm2_gain.astype(jnp.float32), norm2_bias.astype(jnp.float32))
    second_cast = second_norm.astype(jnp.bfloat16)
    hidden_pre = matmul_plain(second_cast, w_fc) + bias_fc.astype(jnp.float32)
    hidden = gelu_tanh(hidden_pre).astype(jnp.bfloat16)
    result = residual + matmul_plain(hidden, w_proj) + bias_proj.astype(jnp.float32)
    outputs = result.astype(jnp.bfloat16).reshape(row_count, length, feature_width)
    stored = (first_scaled, first_inverse, first_cast, projected, logsum, attended, attended_cast, second_scaled, second_inverse, second_cast, hidden_pre, hidden, allowed)
    return (outputs, stored)

def layer_backward(cotangent, params, stored):
    norm1_gain, norm1_bias, w_qkv, bias_qv, w_out, bias_out, norm2_gain, norm2_bias, w_fc, bias_fc, w_proj, bias_proj = params
    first_scaled, first_inverse, first_cast, projected, logsum, attended, attended_cast, second_scaled, second_inverse, second_cast, hidden_pre, hidden, allowed = stored
    row_count, length, feature_width = cotangent.shape
    head_count = feature_width // HEAD_DIM
    token_count = row_count * length
    upstream_cast = cotangent.reshape(token_count, feature_width)
    upstream = upstream_cast.astype(jnp.float32)
    grad_w_proj = matmul_left(hidden, upstream_cast)
    grad_bias_proj = lax.optimization_barrier(jnp.sum(upstream, axis=0))
    grad_hidden = matmul_right(upstream_cast, w_proj) * gelu_slope(hidden_pre)
    grad_hidden_cast = grad_hidden.astype(jnp.bfloat16)
    grad_w_fc = matmul_left(second_cast, grad_hidden_cast)
    grad_bias_fc = lax.optimization_barrier(jnp.sum(grad_hidden, axis=0))
    second_back, grad_norm2_gain, grad_norm2_bias = norm_backward(matmul_right(grad_hidden_cast, w_fc), second_scaled, second_inverse, norm2_gain.astype(jnp.float32))
    grad_residual = upstream + second_back
    grad_residual_cast = grad_residual.astype(jnp.bfloat16)
    grad_w_out = matmul_left(attended_cast, grad_residual_cast)
    grad_bias_out = lax.optimization_barrier(jnp.sum(grad_residual, axis=0))
    grad_attended = matmul_right(grad_residual_cast, w_out).astype(jnp.bfloat16).reshape(row_count, length, head_count, HEAD_DIM)
    split_qkv = projected.reshape(row_count, length, 3, head_count, HEAD_DIM)
    queries, keyed, values = (split_qkv[:, :, 0], split_qkv[:, :, 1], split_qkv[:, :, 2])
    scores = masked_scores(queries, keyed, allowed)
    exact_probs = jnp.exp(scores - logsum)
    attn_probs = exact_probs.astype(jnp.bfloat16)
    grad_probs = batched('rqhd,rkhd->rhqk', grad_attended, values)
    row_delta = lax.optimization_barrier(jnp.sum(grad_attended.astype(jnp.float32) * attended.reshape(row_count, length, head_count, HEAD_DIM), axis=-1))
    row_delta = jnp.transpose(row_delta, (0, 2, 1))[:, :, :, None]
    grad_scores = (exact_probs * (grad_probs - row_delta) * HEAD_DIM ** (-0.5)).astype(jnp.bfloat16)
    grad_queries = batched('rhqk,rkhd->rqhd', grad_scores, keyed)
    grad_keyed = batched('rhqk,rqhd->rkhd', grad_scores, queries)
    grad_values = batched('rhqk,rqhd->rkhd', attn_probs, grad_attended)
    grad_projected = jnp.stack([grad_queries, grad_keyed, grad_values], axis=2).reshape(token_count, 3 * feature_width)
    grad_bias_qv = jnp.concatenate([lax.optimization_barrier(jnp.sum(grad_projected[:, :feature_width], axis=0)), lax.optimization_barrier(jnp.sum(grad_projected[:, 2 * feature_width:], axis=0))])
    grad_projected_cast = grad_projected.astype(jnp.bfloat16)
    grad_w_qkv = matmul_left(first_cast, grad_projected_cast)
    first_back, grad_norm1_gain, grad_norm1_bias = norm_backward(matmul_right(grad_projected_cast, w_qkv), first_scaled, first_inverse, norm1_gain.astype(jnp.float32))
    input_grad = (grad_residual + first_back).reshape(row_count, length, feature_width)
    grads = (grad_norm1_gain, grad_norm1_bias, grad_w_qkv, grad_bias_qv, grad_w_out, grad_bias_out, grad_norm2_gain, grad_norm2_bias, grad_w_fc, grad_bias_fc, grad_w_proj, grad_bias_proj)
    return (input_grad, grads)

def reference(inputs, segments, cotangent, norm1_gain, norm1_bias, w_qkv, bias_qv, w_out, bias_out, norm2_gain, norm2_bias, w_fc, bias_fc, w_proj, bias_proj):
    params = (norm1_gain, norm1_bias, w_qkv, bias_qv, w_out, bias_out, norm2_gain, norm2_bias, w_fc, bias_fc, w_proj, bias_proj)
    block_rows = math.gcd(ROWS, max(1, 4096 // TOK_DEV))
    block_count = ROWS // block_rows

    def scan_step(totals, slices):
        block_inputs, block_segments, block_cotangent = slices
        block_out, stored = layer_forward(block_inputs, block_segments, params)
        block_grad, grads = layer_backward(block_cotangent, params, stored)
        return (jax.tree.map(lambda summed, addend: summed + addend, totals, grads), (block_out, block_grad))
    initial = tuple((jnp.zeros(param.shape, jnp.float32) for param in params))
    totals, (all_out, all_grad) = lax.scan(scan_step, initial, (inputs.reshape(block_count, block_rows, TOK_DEV, D), segments.reshape(block_count, block_rows, TOK_DEV), cotangent.reshape(block_count, block_rows, TOK_DEV, D)))
    return (all_out.reshape(ROWS, TOK_DEV, D), all_grad.reshape(ROWS, TOK_DEV, D), totals[0], totals[1], totals[2], totals[3], totals[4], totals[5], totals[6], totals[7], totals[8], totals[9], totals[10], totals[11])
```

```python
import jax
import jax.numpy as jnp
from jax import lax
from jax.sharding import PartitionSpec as P

HEAD_DIM = 64


EPSILON = 1e-05
GELU_SCALE = 0.7978845608028654
CUBIC_TERM = 0.044715


def matmul_plain(left_side, right_side):
    return jnp.dot(left_side, right_side, preferred_element_type=jnp.float32)


def matmul_left(left_side, right_side):
    return lax.dot_general(
        left_side, right_side, (((0,), (0,)), ((), ())), preferred_element_type=jnp.float32
    )


def matmul_right(left_side, right_side):
    return lax.dot_general(
        left_side, right_side, (((1,), (1,)), ((), ())), preferred_element_type=jnp.float32
    )


def batched(form, left_side, right_side):
    return jnp.einsum(form, left_side, right_side, preferred_element_type=jnp.float32)


def norm_forward(values, norm_gain, offset):
    center = values - jnp.mean(values, axis=-1, keepdims=True)
    inverse = lax.rsqrt(jnp.mean(center * center, axis=-1, keepdims=True) + EPSILON)
    scaled = center * inverse
    return (scaled * norm_gain + offset, scaled, inverse)


def norm_backward(upstream, scaled, inverse, norm_gain):
    weighted = upstream * norm_gain
    result = inverse * (
        weighted
        - jnp.mean(weighted, axis=-1, keepdims=True)
        - scaled * jnp.mean(weighted * scaled, axis=-1, keepdims=True)
    )
    return (result, jnp.sum(upstream * scaled, axis=0), jnp.sum(upstream, axis=0))


def gelu_both(values):
    tangent = jnp.tanh(GELU_SCALE * (values + CUBIC_TERM * values * values * values))
    value = 0.5 * values * (1.0 + tangent)
    slope = 0.5 * (1.0 + tangent) + 0.5 * values * (1.0 - tangent * tangent) * GELU_SCALE * (
        1.0 + 3.0 * CUBIC_TERM * values * values
    )
    return value, slope


def allowed_mask(segments):
    positions = jnp.arange(segments.shape[1])
    causal = positions[:, None] >= positions[None, :]
    same_segment = segments[:, :, None] == segments[:, None, :]
    return (same_segment & causal[None, :, :])[:, None, :, :]


def masked_scores(queries, keyed, allowed):
    raw = batched("rqhd,rkhd->rhqk", queries, keyed) * HEAD_DIM ** (-0.5)
    return jnp.where(allowed, raw, -1e30)


def swap(value, axis, mask):
    size = lax.axis_size(axis)
    return lax.ppermute(value, axis, [(i, i ^ mask) for i in range(size)])


def after(value, *earlier):
    return lax.optimization_barrier((value, *earlier))[0]


def column_cuts(width, count):
    step = -(-width // (count * 256)) * 256
    edges = list(range(0, width, step)) + [width]
    return list(zip(edges[:-1], edges[1:]))


def gather_tokens(value):
    far = swap(value, "group", 2)
    return jnp.concatenate([value, swap(value, "group", 1), far, swap(far, "group", 1)], axis=0)


def trade_columns(value, rows):
    group = lax.axis_index("group")
    blocks = [
        lax.dynamic_slice_in_dim(value, (group ^ i) * rows, rows, axis=1) for i in range(4)
    ]
    return jnp.concatenate([blocks[0]] + [swap(blocks[i], "group", i) for i in (1, 2, 3)], axis=0)


def trade_tokens(value):
    group = lax.axis_index("group")
    rows = value.shape[0] // 4
    blocks = [value[i * rows : (i + 1) * rows] for i in range(4)]
    blocks = [blocks[0]] + [swap(blocks[i], "group", i) for i in (1, 2, 3)]
    whole = jnp.zeros((4,) + blocks[0].shape, value.dtype)
    for i, block in enumerate(blocks):
        whole = lax.dynamic_update_slice(whole, block[None], (group ^ i, 0, 0))
    return jnp.transpose(whole, (1, 0, 2)).reshape(rows, 4 * value.shape[1])


def scatter_tokens(partial):
    rows = partial.shape[0] // 4
    own, near, far, corner = [partial[i * rows : (i + 1) * rows] for i in range(4)]
    near, corner = swap(near, "group", 1), swap(corner, "group", 1)
    return own + near + swap((far + corner).astype(jnp.bfloat16), "group", 2).astype(jnp.float32)


def pick(bit, first, second):
    return jnp.where(bit == 0, first, second)


def sum_gradient(left, right, masks):
    replica = lax.axis_index("replica")
    bit_a = (replica & masks[0]) // masks[0]
    bit_b = (replica & masks[1]) // masks[1]

    def partial(bit):
        parts = [matmul_left(pick(bit, *pair), cols) for pair, cols in zip(left, right)]
        return parts[0] if len(parts) == 1 else jnp.concatenate(parts, axis=1)

    sent = partial(1 - bit_a).astype(jnp.bfloat16)
    kept = partial(bit_a)
    kept = kept + swap(sent, "replica", masks[0]).astype(jnp.float32)
    middle = kept.shape[1] // 2
    if middle % 128:
        middle = kept.shape[0] // 2
        low, high = kept[:middle], kept[middle:]
    else:
        low, high = kept[:, :middle], kept[:, middle:]
    sent = pick(bit_b, high, low).astype(jnp.bfloat16)
    total = pick(bit_b, low, high) + swap(sent, "replica", masks[1]).astype(jnp.float32)
    mask = 1
    while mask < lax.axis_size("replica"):
        if mask not in masks:
            rounded = total.astype(jnp.bfloat16)
            total = rounded.astype(jnp.float32) + swap(rounded, "replica", mask).astype(jnp.float32)
        mask *= 2
    own = total.astype(jnp.bfloat16)
    beside = swap(own, "replica", masks[1])
    across = swap(own, "replica", masks[0])
    corner = swap(beside, "replica", masks[0])
    join_axis = 0 if own.shape[1] == kept.shape[1] else 1
    near = jnp.concatenate([pick(bit_b, own, beside), pick(bit_b, beside, own)], axis=join_axis)
    far = jnp.concatenate([pick(bit_b, across, corner), pick(bit_b, corner, across)], axis=join_axis)
    whole = jnp.stack([pick(bit_a, near, far), pick(bit_a, far, near)], axis=0)
    return whole.reshape(2 * kept.shape[0], kept.shape[1]).astype(jnp.float32)


def row_halves(value):
    middle = value.shape[1] // 2
    return value[:, :middle], value[:, middle:]


def sum_everywhere(value):
    for axis in ("group", "replica"):
        mask = 1
        while mask < lax.axis_size(axis):
            value = value + swap(value, axis, mask)
            mask *= 2
    return value


def per_device(
    inputs,
    segments,
    cotangent,
    norm1_gain,
    norm1_bias,
    w_qkv,
    bias_qv,
    w_out,
    bias_out,
    norm2_gain,
    norm2_bias,
    w_fc,
    bias_fc,
    w_proj,
    bias_proj,
):
    group = lax.axis_index("group")
    vectors = (norm1_gain, norm1_bias, bias_qv, bias_out, norm2_gain, norm2_bias, bias_fc, bias_proj)
    packed = jnp.concatenate(vectors)[None]
    packed = [packed] + [swap(packed, "group", i) for i in (1, 2, 3)]
    low, high = pick(group & 1, packed[0], packed[1]), pick(group & 1, packed[1], packed[0])
    far_low, far_high = pick(group & 1, packed[2], packed[3]), pick(group & 1, packed[3], packed[2])
    packed = jnp.concatenate(
        [
            pick(group & 2, low, far_low),
            pick(group & 2, high, far_high),
            pick(group & 2, far_low, low),
            pick(group & 2, far_high, high),
        ],
        axis=0,
    )
    full, start = [], 0
    for vector in vectors:
        full.append(packed[:, start : start + vector.shape[0]].reshape(-1).astype(jnp.float32))
        start += vector.shape[0]
    gain1, offset1, offset_qv, offset_out, gain2, offset2, offset_fc, offset_proj = full

    qkv_rows, out_rows, fc_rows, proj_rows = [w.shape[0] for w in (w_qkv, w_out, w_fc, w_proj)]
    qkv_width = w_qkv.shape[1]
    upstream_cast = cotangent.reshape(-1, cotangent.shape[-1])
    row_count, length, feature_width = inputs.shape
    head_count = feature_width // HEAD_DIM
    token_count = row_count * length
    tokens = inputs.reshape(token_count, feature_width).astype(jnp.float32)
    first_norm, first_scaled, first_inverse = norm_forward(tokens, gain1, offset1)
    first_cast = first_norm.astype(jnp.bfloat16)
    qkv_bias = jnp.concatenate(
        [
            offset_qv[:feature_width],
            jnp.zeros((feature_width,), jnp.float32),
            offset_qv[feature_width:],
        ]
    )
    first_mine = trade_columns(first_cast, qkv_rows)
    projected = (scatter_tokens(matmul_plain(first_mine, w_qkv)) + qkv_bias).astype(jnp.bfloat16)
    upstream_all = gather_tokens(after(upstream_cast, projected))
    product = trade_tokens(matmul_right(upstream_all, w_proj).astype(jnp.bfloat16))
    split_qkv = projected.reshape(row_count, length, 3, head_count, HEAD_DIM)
    queries, keyed, values = (split_qkv[:, :, 0], split_qkv[:, :, 1], split_qkv[:, :, 2])
    allowed = allowed_mask(segments)
    scores = masked_scores(queries, keyed, allowed)
    row_peak = jnp.max(scores, axis=-1, keepdims=True)
    logsum = row_peak + jnp.log(jnp.sum(jnp.exp(scores - row_peak), axis=-1, keepdims=True))
    exact_probs = jnp.exp(scores - logsum)
    attn_probs = exact_probs.astype(jnp.bfloat16)
    attended = batched("rhqk,rkhd->rqhd", attn_probs, values).reshape(token_count, feature_width)
    attended_cast = attended.astype(jnp.bfloat16)
    attended_mine = trade_columns(attended_cast, out_rows)
    residual = tokens + scatter_tokens(matmul_plain(attended_mine, w_out)) + offset_out
    second_norm, second_scaled, second_inverse = norm_forward(residual, gain2, offset2)
    second_cast = second_norm.astype(jnp.bfloat16)
    second_mine = trade_columns(second_cast, fc_rows)
    hidden_pre = scatter_tokens(matmul_plain(second_mine, w_fc)) + offset_fc
    hidden_value, hidden_slope = gelu_both(hidden_pre)
    hidden = hidden_value.astype(jnp.bfloat16)

    hidden_mine = trade_columns(hidden, proj_rows)
    rows = row_halves(hidden_mine)
    grad_w_proj = jnp.concatenate(
        [sum_gradient([row_halves(part)], [upstream_all], (1, 2)) for part in rows], axis=0
    )

    upstream = upstream_cast.astype(jnp.float32)
    grad_bias_proj = jnp.sum(upstream, axis=0)
    grad_hidden = product.astype(jnp.float32) * hidden_slope
    grad_hidden_cast = grad_hidden.astype(jnp.bfloat16)
    grad_bias_fc = jnp.sum(grad_hidden, axis=0)
    grad_hidden_all = gather_tokens(grad_hidden_cast)
    grad_w_fc = jnp.concatenate(
        [
            sum_gradient([row_halves(second_mine)], [grad_hidden_all[:, start:end]], masks)
            for (start, end), masks in zip(column_cuts(w_fc.shape[1], 2), ((1, 2), (2, 1)))
        ],
        axis=1,
    )
    second_back, grad_norm2_gain, grad_norm2_bias = norm_backward(
        trade_tokens(matmul_right(grad_hidden_all, w_fc)), second_scaled, second_inverse, gain2
    )
    grad_residual = upstream + second_back
    grad_residual_cast = grad_residual.astype(jnp.bfloat16)
    grad_bias_out = jnp.sum(grad_residual, axis=0)
    grad_residual_all = gather_tokens(grad_residual_cast)
    grad_attended = trade_tokens(
        matmul_right(grad_residual_all, w_out).astype(jnp.bfloat16)
    ).reshape(row_count, length, head_count, HEAD_DIM)
    grad_probs = batched("rqhd,rkhd->rhqk", grad_attended, values)
    row_delta = jnp.sum(
        grad_attended.astype(jnp.float32)
        * attended.reshape(row_count, length, head_count, HEAD_DIM),
        axis=-1,
    )
    row_delta = jnp.transpose(row_delta, (0, 2, 1))[:, :, :, None]
    grad_scores = (exact_probs * (grad_probs - row_delta) * HEAD_DIM ** (-0.5)).astype(jnp.bfloat16)
    grad_queries = batched("rhqk,rkhd->rqhd", grad_scores, keyed)
    grad_keyed = batched("rhqk,rqhd->rkhd", grad_scores, queries)
    grad_values = batched("rhqk,rqhd->rkhd", attn_probs, grad_attended)
    grad_projected = jnp.stack([grad_queries, grad_keyed, grad_values], axis=2).reshape(
        token_count, 3 * feature_width
    )
    grad_bias_qv = jnp.concatenate(
        [
            jnp.sum(grad_projected[:, :feature_width], axis=0),
            jnp.sum(grad_projected[:, 2 * feature_width :], axis=0),
        ]
    )
    grad_projected_cast = grad_projected.astype(jnp.bfloat16)
    grad_projected_all = gather_tokens(grad_projected_cast)
    cut = column_cuts(qkv_width + w_out.shape[1], 2)[0][1]
    grad_head = sum_gradient([row_halves(first_mine)], [grad_projected_all[:, :cut]], (1, 2))
    grad_tail = sum_gradient(
        [row_halves(first_mine), row_halves(attended_mine)],
        [grad_projected_all[:, cut:], grad_residual_all], (2, 1)
    )
    grad_w_qkv = jnp.concatenate([grad_head, grad_tail[:, : qkv_width - cut]], axis=1)
    grad_w_out = grad_tail[:, qkv_width - cut :]
    first_back, grad_norm1_gain, grad_norm1_bias = norm_backward(
        trade_tokens(matmul_right(grad_projected_all, w_qkv)), first_scaled, first_inverse, gain1
    )
    input_grad = (grad_residual + first_back).reshape(row_count, length, feature_width)

    grad_vectors = (
        grad_norm1_gain,
        grad_norm1_bias,
        grad_bias_qv,
        grad_bias_out,
        grad_norm2_gain,
        grad_norm2_bias,
        grad_bias_fc,
        grad_bias_proj,
    )
    vector_sums = sum_everywhere(jnp.concatenate(grad_vectors))
    owned, start = [], 0
    for vector, whole in zip(vectors, grad_vectors):
        size = vector.shape[0]
        owned.append(lax.dynamic_slice_in_dim(vector_sums, start + group * size, size))
        start += whole.shape[0]

    result = residual + scatter_tokens(matmul_plain(hidden_mine, w_proj)) + offset_proj
    outputs = result.astype(jnp.bfloat16).reshape(row_count, length, feature_width)
    return (
        outputs,
        input_grad,
        owned[0],
        owned[1],
        grad_w_qkv,
        owned[2],
        grad_w_out,
        owned[3],
        owned[4],
        owned[5],
        grad_w_fc,
        owned[6],
        grad_w_proj,
        owned[7],
    )


def solution(mesh):
    return jax.shard_map(
        per_device,
        mesh=mesh,
        in_specs=(
            P(("group", "replica"), None, None),
            P(("group", "replica"), None),
            P(("group", "replica"), None, None),
            P("group"),
            P("group"),
            P("group", None),
            P("group"),
            P("group", None),
            P("group"),
            P("group"),
            P("group"),
            P("group", None),
            P("group"),
            P("group", None),
            P("group"),
        ),
        out_specs=(
            P(("group", "replica"), None, None),
            P(("group", "replica"), None, None),
            P("group"),
            P("group"),
            P("group", None),
            P("group"),
            P("group", None),
            P("group"),
            P("group"),
            P("group"),
            P("group", None),
            P("group"),
            P("group", None),
            P("group"),
        ),
        check_vma=False,
    )
```
